32 devices in a mesh: dp: 2 (over x), tp: 16 (over y, z, core).
Axes of the slice: x: 2, y: 2, z: 4, core: 2. Of those that a mesh axis runs over, the one named last changes fastest.
Arguments:
- x: bfloat16 [256, 8192], P('dp'), parts along dimension 0
- w_gate: bfloat16 [8192, 32768], P(None, 'tp')
- w_up: bfloat16 [8192, 32768], P(None, 'tp')
- w_down: bfloat16 [32768, 8192], P('tp')
Outputs:
- output: bfloat16 [256, 8192], P('dp'), parts along dimension 0
There are 2 independent parts. The reference program is written for one: setup_inputs(seed, part) draws one part's arguments, and reference() takes and returns one part's arrays. A program takes and returns all parts, laid end to end along the dimension named above; an argument that names none is the same for every part.
All inputs are finite; a program needn't handle non-finite values.
Results may differ from the reference program's by a relative error of at most 0.016.
Values are sent between devices in bfloat16 or wider.
A program may use at most 2 GiB of HBM per device.

```python
import jax
import jax.numpy as jnp

ROWS = 128
D = 8192
FF = 32768


def setup_inputs(seed: int = 0, part: int = 0) -> dict:
    kx, kg, ku, kd = jax.random.split(jax.random.key(seed), 4)
    drawn = {
        "x": jax.random.normal(jax.random.fold_in(kx, part), (ROWS, D), jnp.float32),
        "w_gate": jax.random.normal(kg, (D, FF), jnp.float32) * D**-0.5,
        "w_up": jax.random.normal(ku, (D, FF), jnp.float32) * D**-0.5,
        "w_down": jax.random.normal(kd, (FF, D), jnp.float32) * FF**-0.5,
    }
    return {k: v.astype(jnp.bfloat16) for k, v in drawn.items()}


def reference(x, w_gate, w_up, w_down):
    gate = jnp.dot(x, w_gate, preferred_element_type=jnp.float32)
    up = jnp.dot(x, w_up, preferred_element_type=jnp.float32)
    hidden = (jax.nn.silu(gate) * up).astype(jnp.bfloat16)
    return jnp.dot(hidden, w_down, preferred_element_type=jnp.float32).astype(jnp.bfloat16)
```

```python
import functools

import jax
import jax.numpy as jnp
from jax import lax
from jax.experimental import pallas as pl
from jax.experimental.pallas import tpu as pltpu
from jax.sharding import PartitionSpec as P

MESH = pl.DeviceIdType.MESH
ROWS = 128
TK = 2048
TN = 512
SLOTS = 14
CORE, Y1, ZZ, ZY, MZ, MY, YZ, FYE, FYY, FZM, FZA, FZB, SY0, SY1, SZ0, SZ1 = range(16)


def kernel(x_hbm, wg_hbm, wu_hbm, wd_hbm, out, xv, wbuf, acc_g, acc_u, h, total,
           cs, cr, ys, yr, zzs, zzr, zys, zyr, mzs, mzr, mys, myr, yzs, yzr,
           xsem, wsem, ssem, rsem):
    dp = lax.axis_index("dp")
    tp = lax.axis_index("tp")
    c = lax.rem(tp, 2)
    z = lax.rem(tp // 2, 4)
    y = tp // 8
    half = z // 2
    inner = (z + 1) // 2 == 1
    ends = jnp.logical_not(inner)
    ff = wg_hbm.shape[1]
    d = wd_hbm.shape[1]
    kx = wg_hbm.shape[0] // TK
    nb = ff // TN
    n_up = 2 * kx * nb
    n_chunks = d // (2 * TN)
    n_steps = n_up + 2 * n_chunks

    def dev(yy, zz, cc):
        return (dp, (yy * 4 + zz) * 2 + cc)

    sib = dev(y, z, 1 - c)
    ynb = dev(1 - y, z, c)
    znb = dev(y, z + 1 - 2 * lax.rem(z, 2), c)
    mid = dev(y, 3 - z, c)

    barrier = pltpu.get_barrier_semaphore()
    for nbr in (sib, ynb, znb):
        pl.semaphore_signal(barrier, inc=1, device_id=nbr, device_id_type=MESH)

    @pl.when(inner)
    def _():
        pl.semaphore_signal(barrier, inc=1, device_id=mid, device_id_type=MESH)

    def tile_copy(ref, k, n, s):
        slot = lax.rem(s, SLOTS)
        return pltpu.make_async_copy(
            ref.at[pl.ds(k * TK, TK), pl.ds(n * TN, TN)], wbuf.at[slot], wsem.at[slot])

    def fetch_up(it):
        b, k = it // kx, lax.rem(it, kx)
        tile_copy(wg_hbm, k, b, 2 * it).start()
        tile_copy(wu_hbm, k, b, 2 * it + 1).start()

    def fetch_down(i):
        tile_copy(wd_hbm, 0, 2 * i, n_up + 2 * i).start()
        tile_copy(wd_hbm, 0, 2 * i + 1, n_up + 2 * i + 1).start()

    def fetch(it):
        @pl.when(it < kx * nb)
        def _():
            fetch_up(it)

        @pl.when(jnp.logical_and(it >= kx * nb, it < n_steps // 2))
        def _():
            fetch_down(it - kx * nb)

    def wait_tile(s):
        slot = lax.rem(s, SLOTS)
        pltpu.make_async_copy(wd_hbm.at[pl.ds(0, TK), pl.ds(0, TN)], wbuf.at[slot], wsem.at[slot]).wait()
        return slot

    def x_copy(k):
        return pltpu.make_async_copy(
            x_hbm.at[:, pl.ds(k * TK, TK)], xv.at[:, pl.ds(k * TK, TK)], xsem.at[k])

    for k in range(kx):
        x_copy(k).start()
        if k < SLOTS // 2 - 1:
            fetch_up(k)
    for k in range(kx, SLOTS // 2 - 1):
        fetch_up(k)

    @pl.loop(0, kx * nb)
    def _(it):
        b, k = it // kx, lax.rem(it, kx)
        fetch(it + SLOTS // 2 - 1)

        @pl.when(it < kx)
        def _():
            x_copy(k).wait()

        xk = xv[:, pl.ds(pl.multiple_of(k * TK, TK), TK)]

        @pl.when(k == 0)
        def _():
            acc_g[...] = jnp.zeros_like(acc_g)
            acc_u[...] = jnp.zeros_like(acc_u)

        slot = wait_tile(2 * it)
        acc_g[...] += jnp.dot(xk, wbuf[slot], preferred_element_type=jnp.float32)
        slot = wait_tile(2 * it + 1)
        acc_u[...] += jnp.dot(xk, wbuf[slot], preferred_element_type=jnp.float32)

        @pl.when(k == kx - 1)
        def _():
            h[:, pl.ds(pl.multiple_of(b * TN, TN), TN)] = (
                jax.nn.silu(acc_g[...]) * acc_u[...]).astype(jnp.bfloat16)

    @pl.when(inner)
    def _():
        pl.semaphore_wait(barrier, 4)

    @pl.when(ends)
    def _():
        pl.semaphore_wait(barrier, 3)

    def send(kind, k, src, dst, to):
        return pltpu.make_async_remote_copy(
            src_ref=src, dst_ref=dst, send_sem=ssem.at[kind, k], recv_sem=rsem.at[kind, k],
            device_id=to, device_id_type=MESH)

    rc = 64 * c
    ry, ry_other = rc + 32 * y, rc + 32 * (1 - y)
    rz, rz_other = rc + 32 * half, rc + 32 * (1 - half)

    def col(k, part):
        return pl.ds(pl.multiple_of(k * 2 * TN + part * TN, TN), TN)

    def rows(r, n):
        return pl.ds(pl.multiple_of(r, 32), n)

    def o(k, part, r):
        return out.at[rows(r, 32), col(k, part)]

    CY, CZ = pl.ds(0, TN), pl.ds(TN, TN)

    def f32(v):
        return v.astype(jnp.float32)

    def bf16(v):
        return v.astype(jnp.bfloat16)

    def core_send(k):
        return send(CORE, k, cs.at[k], cr.at[k], sib)

    def y1_send(k):
        return send(Y1, k, ys.at[k], yr.at[k], ynb)

    def zz_send(k):
        return send(ZZ, k, zzs.at[k], zzr.at[k], znb)

    def zy_send(k):
        return send(ZY, k, zys.at[k], zyr.at[k], znb)

    def mz_send(k):
        return send(MZ, k, mzs.at[k], mzr.at[k], mid)

    def my_send(k):
        return send(MY, k, mys.at[k], myr.at[k], mid)

    def yz_send(k):
        return send(YZ, k, yzs.at[k], yzr.at[k], ynb)

    def final(kind, k, part, r, to):
        return send(kind, k, o(k, part, r), o(k, part, r), to)

    def compute(k):
        for part in range(2):
            slot = wait_tile(n_up + 2 * k + part)
            total[k, :, part * TN:(part + 1) * TN] = jnp.dot(
                h[...], wbuf[slot], preferred_element_type=jnp.float32)
        cs[k] = bf16(total[k, rows(64 - rc, 64), :])
        core_send(k).start()

    def stage1(k):
        core_send(k).wait_recv()
        total[k, rows(rc, 64), :] += f32(cr[k])
        ys[k] = bf16(total[k, rows(ry_other, 32), CY])
        y1_send(k).start()

        @pl.when(ends)
        def _():
            zzs[k] = bf16(total[k, rows(rc, 64), CZ])
            zz_send(k).start()

    def stage2(k):
        @pl.when(inner)
        def _():
            zz_send(k).wait_recv()
            total[k, rows(rc, 64), CZ] += f32(zzr[k])
            mzs[k] = bf16(total[k, rows(rz_other, 32), CZ])
            mz_send(k).start()
            y1_send(k).wait_recv()
            total[k, rows(ry, 32), CY] += f32(yr[k])

        @pl.when(ends)
        def _():
            y1_send(k).wait_recv()
            zys[k] = bf16(total[k, rows(ry, 32), CY] + f32(yr[k]))
            zy_send(k).start()

    def stage3(k):
        @pl.when(inner)
        def _():
            mz_send(k).wait_recv()
            yzs[k] = bf16(total[k, rows(rz, 32), CZ] + f32(mzr[k]))
            yz_send(k).start()
            zy_send(k).wait_recv()
            mys[k] = bf16(total[k, rows(ry, 32), CY] + f32(zyr[k]))
            my_send(k).start()

    def stage4(k):
        @pl.when(inner)
        def _():
            yz_send(k).wait_recv()
            out[rows(rz, 32), col(k, 1)] = bf16(f32(yzs[k]) + f32(yzr[k]))
            final(FZM, k, 1, rz, mid).start()
            final(FZA, k, 1, rz, znb).start()
            final(SZ0, k, 1, rz, sib).start()
            my_send(k).wait_recv()
            out[rows(ry, 32), col(k, 0)] = bf16(f32(mys[k]) + f32(myr[k]))
            final(FYE, k, 0, ry, znb).start()
            final(FYY, k, 0, ry, ynb).start()
            final(SY0, k, 0, ry, sib).start()

    def stage5(k):
        @pl.when(inner)
        def _():
            final(FZM, k, 1, rz_other, mid).wait_recv()
            final(FZB, k, 1, rz_other, znb).start()
            final(SZ1, k, 1, rz_other, sib).start()
            final(FYY, k, 0, ry_other, ynb).wait_recv()
            final(SY1, k, 0, ry_other, sib).start()

        @pl.when(ends)
        def _():
            final(FZA, k, 1, rz, znb).wait_recv()
            final(SZ0, k, 1, rz, sib).start()
            final(FYE, k, 0, ry, znb).wait_recv()
            final(FYY, k, 0, ry, ynb).start()
            final(SY0, k, 0, ry, sib).start()

    def stage6(k):
        @pl.when(ends)
        def _():
            final(FZB, k, 1, rz_other, znb).wait_recv()
            final(SZ1, k, 1, rz_other, sib).start()
            final(FYY, k, 0, ry_other, ynb).wait_recv()
            final(SY1, k, 0, ry_other, sib).start()

    def at(k, fn):
        @pl.when(jnp.logical_and(k >= 0, k < n_chunks))
        def _():
            fn(k)

    @pl.loop(0, n_chunks + DELAYS[-1])
    def _(i):
        at(i - DELAYS[5], stage6)
        at(i - DELAYS[4], stage5)
        at(i - DELAYS[3], stage4)
        at(i - DELAYS[2], stage3)
        at(i - DELAYS[1], stage2)

        @pl.when(i < n_chunks)
        def _():
            fetch(i + kx * nb + SLOTS // 2 - 1)
            compute(i)

        at(i - DELAYS[0], stage1)

    rs, rs_y, rs_yo, rs_z, rs_zo = 64 - rc, 64 - rc + 32 * y, 64 - rc + 32 * (1 - y), 64 - rc + 32 * half, 64 - rc + 32 * (1 - half)

    @pl.loop(0, n_chunks)
    def _(k):
        final(SZ0, k, 1, rs_z, sib).wait_recv()
        final(SZ1, k, 1, rs_zo, sib).wait_recv()
        final(SY0, k, 0, rs_y, sib).wait_recv()
        final(SY1, k, 0, rs_yo, sib).wait_recv()
        core_send(k).wait_send()
        y1_send(k).wait_send()
        final(SZ0, k, 1, rz, sib).wait_send()
        final(SZ1, k, 1, rz_other, sib).wait_send()
        final(SY0, k, 0, ry, sib).wait_send()
        final(SY1, k, 0, ry_other, sib).wait_send()
        final(FYY, k, 0, ry, ynb).wait_send()

        @pl.when(inner)
        def _():
            mz_send(k).wait_send()
            my_send(k).wait_send()
            yz_send(k).wait_send()
            final(FYE, k, 0, ry, znb).wait_send()
            final(FZM, k, 1, rz, mid).wait_send()
            final(FZA, k, 1, rz, znb).wait_send()
            final(FZB, k, 1, rz_other, znb).wait_send()

        @pl.when(ends)
        def _():
            zz_send(k).wait_send()
            zy_send(k).wait_send()


DELAYS = (1, 3, 5, 7, 9, 11)


def mlp(x, wg, wu, wd):
    rows, d = x.shape
    ff = wg.shape[1]
    nc = d // (2 * TN)
    bf, f4 = jnp.bfloat16, jnp.float32
    any_spec = pl.BlockSpec(memory_space=pl.ANY)
    small = [pltpu.VMEM((nc, 32, TN), bf)] * 2
    return pl.pallas_call(
        kernel,
        out_shape=jax.ShapeDtypeStruct((rows, d), bf),
        in_specs=[any_spec] * 4,
        out_specs=pl.BlockSpec(memory_space=pltpu.VMEM),
        scratch_shapes=[
            pltpu.VMEM((rows, d), bf),
            pltpu.VMEM((SLOTS, TK, TN), bf),
            pltpu.VMEM((rows, TN), f4),
            pltpu.VMEM((rows, TN), f4),
            pltpu.VMEM((rows, ff), bf),
            pltpu.VMEM((nc, rows, 2 * TN), f4),
            pltpu.VMEM((nc, rows // 2, 2 * TN), bf),
            pltpu.VMEM((nc, rows // 2, 2 * TN), bf),
            *small,
            pltpu.VMEM((nc, rows // 2, TN), bf),
            pltpu.VMEM((nc, rows // 2, TN), bf),
            *small,
            *small,
            *small,
            *small,
            pltpu.SemaphoreType.DMA((d // TK,)),
            pltpu.SemaphoreType.DMA((SLOTS,)),
            pltpu.SemaphoreType.DMA((16, nc)),
            pltpu.SemaphoreType.DMA((16, nc)),
        ],
        compiler_params=pltpu.CompilerParams(
            collective_id=0, has_side_effects=True, vmem_limit_bytes=60 << 20),
        cost_estimate=pl.CostEstimate(
            flops=6 * rows * d * ff, bytes_accessed=6 * d * ff, transcendentals=rows * ff),
    )(x, wg, wu, wd)


def solution(mesh):
    return jax.shard_map(
        mlp,
        mesh=mesh,
        in_specs=(P("dp", None), P(None, "tp"), P(None, "tp"), P("tp", None)),
        out_specs=P("dp", None),
        check_vma=False,
    )
```
